8 devices in a mesh: rep: 1 (over z), tp: 2 (over y), sp: 4 (over x, core).
Axes of the slice: x: 2, y: 2, z: 1, core: 2. Of those that a mesh axis runs over, the one named last changes fastest.
Arguments:
- x_tokens: bfloat16 [4096, 4096], P(('rep', 'sp'))
- positions: int32 [4096], P(('rep', 'sp'))
- gains: float32 [2, 4, 4096], replicated
- w_q: bfloat16 [2, 4096, 32, 128], P(None, None, 'tp')
- w_k: bfloat16 [2, 4096, 8, 128], P(None, None, 'tp')
- w_v: bfloat16 [2, 4096, 8, 128], P(None, None, 'tp')
- w_o: bfloat16 [2, 32, 128, 4096], P(None, 'tp')
- w_gate: bfloat16 [2, 4096, 12288], P(None, None, 'tp')
- w_up: bfloat16 [2, 4096, 12288], P(None, None, 'tp')
- w_down: bfloat16 [2, 12288, 4096], P(None, 'tp')
Outputs:
- output 1: bfloat16 [4096, 4096], P(('rep', 'sp'))
- output 2: bfloat16 [512, 8, 128], P('rep', ('tp', 'sp'))
- output 3: bfloat16 [512, 8, 128], P('rep', ('tp', 'sp'))
- output 4: bfloat16 [4096, 8, 128], P('rep', ('tp', 'sp'))
- output 5: bfloat16 [4096, 8, 128], P('rep', ('tp', 'sp'))
All inputs are finite; a program needn't handle non-finite values.
Results may differ from the reference program's by a relative error of at most 0.0162272.
Values are sent between devices in bfloat16 or wider.
A program may use at most 1.75 GiB of HBM per device.

```python
import jax
import jax.numpy as jnp
from jax import lax

D = 4096
HEADS = 32
KV_HEADS = 8
HEAD = 128
FF = 12288
TOKENS = 4096
WINDOW = 512
CACHE_HEADS = 8
REF_BLOCK = 64

GROUP_SIZE = HEADS // KV_HEADS
REPEAT = CACHE_HEADS // KV_HEADS
NORM_EPS = 1e-6
LOCAL_BASE = 10000.0
GLOBAL_BASE = 1000000.0


def setup_inputs(seed: int = 0, part: int = 0) -> dict:
    part_key = jax.random.fold_in(jax.random.key(seed), part)
    key_x, key_pos = jax.random.split(part_key, 2)
    weight_keys = jax.random.split(jax.random.key(seed + 1), 8)
    x_tokens = jax.random.normal(key_x, (TOKENS, D), jnp.float32).astype(jnp.bfloat16)
    start = jax.random.randint(key_pos, (), 0, 4096)
    positions = (start + jnp.arange(TOKENS)).astype(jnp.int32)
    gains = 1.0 + 0.25 * jax.random.normal(weight_keys[0], (2, 4, D), jnp.float32)

    def weight(key, shape, fan_in):
        return (jax.random.normal(key, shape, jnp.float32) * fan_in ** -0.5).astype(jnp.bfloat16)

    return {
        'x_tokens': x_tokens,
        'positions': positions,
        'gains': gains,
        'w_q': weight(weight_keys[1], (2, D, HEADS, HEAD), D),
        'w_k': weight(weight_keys[2], (2, D, KV_HEADS, HEAD), D),
        'w_v': weight(weight_keys[3], (2, D, KV_HEADS, HEAD), D),
        'w_o': weight(weight_keys[4], (2, HEADS, HEAD, D), HEADS * HEAD),
        'w_gate': weight(weight_keys[5], (2, D, FF), D),
        'w_up': weight(weight_keys[6], (2, D, FF), D),
        'w_down': weight(weight_keys[7], (2, FF, D), FF),
    }


def rms_norm(values, gain):
    wide = values.astype(jnp.float32)
    inv_rms = lax.rsqrt(jnp.mean(wide * wide, axis=-1, keepdims=True) + NORM_EPS)
    return wide * inv_rms * gain


def rotary(projected, positions, base):
    half = projected.shape[-1] // 2
    inv_freq = base ** (-jnp.arange(half, dtype=jnp.float32) / half)
    angles = positions.astype(jnp.float32)[..., None] * inv_freq
    cos_part = jnp.cos(angles)[..., None, :]
    sin_part = jnp.sin(angles)[..., None, :]
    first = projected[..., :half]
    second = projected[..., half:]
    return jnp.concatenate([first * cos_part - second * sin_part, second * cos_part + first * sin_part], axis=-1)


def attention(q_rot, k_rot, v_new, local):
    q_wide = q_rot.reshape(TOKENS, KV_HEADS, GROUP_SIZE, HEAD).astype(jnp.float32)
    k_wide = k_rot.astype(jnp.float32)
    v_wide = v_new.astype(jnp.float32)
    span = WINDOW + REF_BLOCK if local else TOKENS

    def one_block(block_id):
        q_start = block_id * REF_BLOCK
        q_tile = lax.dynamic_slice_in_dim(q_wide, q_start, REF_BLOCK, 0)
        q_idx = q_start + jnp.arange(REF_BLOCK)
        k_start = jnp.clip(q_start - WINDOW, 0, TOKENS - span) if local else 0
        k_tile = lax.dynamic_slice_in_dim(k_wide, k_start, span, 0)
        v_tile = lax.dynamic_slice_in_dim(v_wide, k_start, span, 0)
        k_idx = k_start + jnp.arange(span)
        allowed = k_idx[None, :] <= q_idx[:, None]
        if local:
            allowed = allowed & (q_idx[:, None] - k_idx[None, :] < WINDOW)
        scores = jnp.einsum('qhgd,khd->hgqk', q_tile, k_tile) * (HEAD ** -0.5)
        weights = jax.nn.softmax(jnp.where(allowed, scores, -1e30), axis=-1)
        weights = weights.astype(jnp.bfloat16).astype(jnp.float32)
        return jnp.einsum('hgqk,khd->qhgd', weights, v_tile).astype(jnp.bfloat16)

    blocks = lax.map(one_block, jnp.arange(TOKENS // REF_BLOCK))
    return blocks.reshape(TOKENS, HEADS * HEAD)


def layer(hidden, positions, gain, w_q, w_k, w_v, w_o, w_gate, w_up, w_down, local):
    base = LOCAL_BASE if local else GLOBAL_BASE
    u_norm = rms_norm(hidden, gain[0]).astype(jnp.bfloat16)
    q_proj = jnp.dot(u_norm, w_q.reshape(D, HEADS * HEAD), preferred_element_type=jnp.float32)
    k_proj = jnp.dot(u_norm, w_k.reshape(D, KV_HEADS * HEAD), preferred_element_type=jnp.float32)
    v_proj = jnp.dot(u_norm, w_v.reshape(D, KV_HEADS * HEAD), preferred_element_type=jnp.float32)
    q_rot = rotary(q_proj.reshape(TOKENS, HEADS, HEAD), positions, base).astype(jnp.bfloat16)
    k_rot = rotary(k_proj.reshape(TOKENS, KV_HEADS, HEAD), positions, base).astype(jnp.bfloat16)
    v_new = v_proj.reshape(TOKENS, KV_HEADS, HEAD).astype(jnp.bfloat16)
    attn_out = attention(q_rot, k_rot, v_new, local)
    o_sum = jnp.dot(attn_out, w_o.reshape(HEADS * HEAD, D), preferred_element_type=jnp.float32)
    x_mid = (hidden.astype(jnp.float32) + rms_norm(o_sum, gain[1])).astype(jnp.bfloat16)
    u_mlp = rms_norm(x_mid, gain[2]).astype(jnp.bfloat16)
    gate_pre = jnp.dot(u_mlp, w_gate, preferred_element_type=jnp.float32)
    up_pre = jnp.dot(u_mlp, w_up, preferred_element_type=jnp.float32)
    hidden_act = (jax.nn.silu(gate_pre) * up_pre).astype(jnp.bfloat16)
    m_sum = jnp.dot(hidden_act, w_down, preferred_element_type=jnp.float32)
    x_out = (x_mid.astype(jnp.float32) + rms_norm(m_sum, gain[3])).astype(jnp.bfloat16)
    k_cache = jnp.repeat(k_rot, REPEAT, axis=1)
    v_cache = jnp.repeat(v_new, REPEAT, axis=1)
    if local:
        return x_out, k_cache[TOKENS - WINDOW:], v_cache[TOKENS - WINDOW:]
    return x_out, k_cache, v_cache


def reference(x_tokens, positions, gains, w_q, w_k, w_v, w_o, w_gate, w_up, w_down):
    hidden, k_local, v_local = layer(x_tokens, positions, gains[0], w_q[0], w_k[0], w_v[0], w_o[0], w_gate[0], w_up[0], w_down[0], True)
    out_hidden, k_global, v_global = layer(hidden, positions, gains[1], w_q[1], w_k[1], w_v[1], w_o[1], w_gate[1], w_up[1], w_down[1], False)
    return out_hidden, k_local, v_local, k_global, v_global
```

```python
import functools
import math

import jax
import jax.numpy as jnp
from jax import lax
from jax.experimental import pallas as pl
from jax.experimental.pallas import tpu as pltpu
from jax.sharding import PartitionSpec as P

F32, BF16 = jnp.float32, jnp.bfloat16
LOG2E = 1.4426950408889634
NEG = -1e30
HEAD = 128
NORM_EPS = 1e-6
WINDOW = 512
LOCAL_BASE = 10000.0
GLOBAL_BASE = 1000000.0
CHUNKS = 2
WO_PIECES = 2
Q_ROWS = 256


def nt(a, b):
    return lax.dot_general(a, b, (((1,), (1,)), ((), ())), preferred_element_type=F32)

def nn(a, b):
    return jnp.dot(a, b, preferred_element_type=F32)

def attn_global_kernel(heads, bq, bk, sc_ref, q_ref, k_ref, v_ref, o_ref, vt_ref, qs_ref, acc_ref, m_ref, l_ref):
    qb = pl.program_id(1)
    code = sc_ref[0]
    q_start = sc_ref[1 + qb]
    c = LOG2E / math.sqrt(128)

    @pl.when(qb == 0)
    def _():
        vt_ref[...] = v_ref[...].T

    for h in range(heads):
        qs_ref[h * bq:(h + 1) * bq, :] = q_ref[:, h * 128:(h + 1) * 128]
    rows = heads * bq
    acc_ref[...] = jnp.zeros_like(acc_ref)
    l_ref[...] = jnp.zeros_like(l_ref)
    m_ref[...] = jnp.full_like(m_ref, NEG)

    def step(kb, masked):
        slot = pl.multiple_of(jnp.bitwise_xor(kb, code) * bk, bk)
        k = k_ref[pl.ds(slot, bk), :]
        s = nt(k, qs_ref[...])
        if masked:
            kt = kb * bk + lax.broadcasted_iota(jnp.int32, (bk, rows), 0)
            qt = q_start + (lax.broadcasted_iota(jnp.int32, (bk, rows), 1) & (bq - 1))
            s = jnp.where(kt <= qt, s, NEG)
        m_old = m_ref[...]
        m_new = jnp.maximum(m_old, jnp.max(s, axis=0, keepdims=True))
        p = jnp.exp2((s - m_new) * c)
        alpha = jnp.exp2((m_old - m_new) * c)
        m_ref[...] = m_new
        l_ref[...] = l_ref[...] * alpha + jnp.sum(p, axis=0, keepdims=True)
        acc_ref[...] = acc_ref[...] * alpha + nn(vt_ref[:, pl.ds(slot, bk)], p.astype(BF16))

    nfull = q_start // bk
    lax.fori_loop(0, nfull, lambda i, _: (step(i, False), 0)[1], 0)
    step(nfull, True)
    out = (acc_ref[...] / l_ref[...]).T
    for h in range(heads):
        o_ref[:, h * 128:(h + 1) * 128] = out[h * bq:(h + 1) * bq, :].astype(BF16)

def attn_global(sc, q, kv, bq=256, bk=512, kvh=4, heads=4):
    T = q.shape[0]; total = kv.shape[0]
    gs = pltpu.PrefetchScalarGridSpec(
        num_scalar_prefetch=1, grid=(kvh, T // bq),
        in_specs=[pl.BlockSpec((bq, heads * 128), lambda g, i, s: (i, g)),
                  pl.BlockSpec((total, 128), lambda g, i, s: (0, g)),
                  pl.BlockSpec((total, 128), lambda g, i, s: (0, kvh + g))],
        out_specs=pl.BlockSpec((bq, heads * 128), lambda g, i, s: (i, g)),
        scratch_shapes=[pltpu.VMEM((128, total), BF16), pltpu.VMEM((heads * bq, 128), BF16),
                        pltpu.VMEM((128, heads * bq), F32), pltpu.VMEM((1, heads * bq), F32), pltpu.VMEM((1, heads * bq), F32)])
    return pl.pallas_call(functools.partial(attn_global_kernel, heads, bq, bk), grid_spec=gs,
        out_shape=jax.ShapeDtypeStruct(q.shape, BF16), name="attn_global",
        cost_estimate=pl.CostEstimate(flops=4 * T * 16 * 128 * total // 2, bytes_accessed=q.size * 4 + kv.size * 2, transcendentals=0),
        compiler_params=pltpu.CompilerParams(dimension_semantics=("arbitrary", "arbitrary")))(sc, q, kv, kv)

def attn_local_kernel(heads, bq, win, sc_ref, q_ref, k_ref, v_ref, o_ref, qs_ref):
    qb = pl.program_id(1)
    first = sc_ref[0]
    c = LOG2E / math.sqrt(128)
    for h in range(heads):
        qs_ref[h * bq:(h + 1) * bq, :] = q_ref[:, h * 128:(h + 1) * 128]
    rows = heads * bq
    span = win + bq
    r0 = pl.multiple_of(qb * bq, bq)
    k = k_ref[pl.ds(r0, span), :]
    s = nt(k, qs_ref[...])
    kt = lax.broadcasted_iota(jnp.int32, (span, rows), 0)
    qt = win + (lax.broadcasted_iota(jnp.int32, (span, rows), 1) & (bq - 1))
    d = qt - kt
    ok = (d >= 0) & (d < win) & (kt + (r0 - win) + first >= 0)
    s = jnp.where(ok, s, NEG)
    m = jnp.max(s, axis=0, keepdims=True)
    p = jnp.exp2((s - m) * c)
    l = jnp.sum(p, axis=0, keepdims=True)
    acc = lax.dot_general(v_ref[pl.ds(r0, span), :], p.astype(BF16), (((0,), (0,)), ((), ())), preferred_element_type=F32)
    out = (acc / l).T
    for h in range(heads):
        o_ref[:, h * 128:(h + 1) * 128] = out[h * bq:(h + 1) * bq, :].astype(BF16)

def attn_local(sc, q, kv, bq=256, win=512, kvh=4, heads=4):
    T = q.shape[0]; total = kv.shape[0]
    gs = pltpu.PrefetchScalarGridSpec(
        num_scalar_prefetch=1, grid=(kvh, T // bq),
        in_specs=[pl.BlockSpec((bq, heads * 128), lambda g, i, s: (i, g)),
                  pl.BlockSpec((total, 128), lambda g, i, s: (0, g)),
                  pl.BlockSpec((total, 128), lambda g, i, s: (0, kvh + g))],
        out_specs=pl.BlockSpec((bq, heads * 128), lambda g, i, s: (i, g)),
        scratch_shapes=[pltpu.VMEM((heads * bq, 128), BF16)])
    return pl.pallas_call(functools.partial(attn_local_kernel, heads, bq, win), grid_spec=gs,
        out_shape=jax.ShapeDtypeStruct(q.shape, BF16), name="attn_local",
        cost_estimate=pl.CostEstimate(flops=4 * T * 16 * 128 * (win + bq), bytes_accessed=q.size * 4 + kv.size * 2, transcendentals=0),
        compiler_params=pltpu.CompilerParams(dimension_semantics=("arbitrary", "arbitrary")))(sc, q, kv, kv)

def qkv_kernel(nk, x_ref, inv_ref, g_ref, wq_ref, wk_ref, wv_ref, cos_ref, sin_ref, q_ref, kv_ref, acc_ref):
    k = pl.program_id(0)
    u = (x_ref[...].astype(F32) * inv_ref[...] * g_ref[...]).astype(BF16)
    bd = u.shape[1]
    wq = wq_ref[0].reshape(bd, -1)
    wk = wk_ref[0].reshape(bd, -1)
    wv = wv_ref[0].reshape(bd, -1)
    nq, nkv = wq.shape[1], wk.shape[1]
    parts = ((0, nq, wq), (nq, nkv, wk), (nq + nkv, nkv, wv))

    @pl.when(k == 0)
    def _():
        for o, n, w in parts:
            acc_ref[:, o:o + n] = nn(u, w)

    @pl.when(k > 0)
    def _():
        for o, n, w in parts:
            acc_ref[:, o:o + n] += nn(u, w)

    @pl.when(k == nk - 1)
    def _():
        cos, sin = cos_ref[...], sin_ref[...]
        for h in range((nq + nkv) // 128):
            t = acc_ref[:, h * 128:(h + 1) * 128]
            r = (t * cos + pltpu.roll(t, 64, 1) * sin).astype(BF16)
            if h * 128 < nq:
                q_ref[:, h * 128:(h + 1) * 128] = r
            else:
                kv_ref[:, h * 128 - nq:(h + 1) * 128 - nq] = r
        kv_ref[:, nkv:] = acc_ref[:, nq + nkv:].astype(BF16)

def qkv(layer, x, inv, gain, w_q, w_k, w_v, cos, sin, bd=256):
    T, D = x.shape
    nq, nkv = w_q.shape[2] * 128, w_k.shape[2] * 128
    hq, hk = w_q.shape[2], w_k.shape[2]
    nk = D // bd
    return pl.pallas_call(functools.partial(qkv_kernel, nk), grid=(nk,),
        in_specs=[pl.BlockSpec((T, bd), lambda k: (0, k)), pl.BlockSpec((T, 1), lambda k: (0, 0)),
                  pl.BlockSpec((1, bd), lambda k: (0, k)),
                  pl.BlockSpec((1, bd, hq, 128), lambda k: (layer, k, 0, 0)),
                  pl.BlockSpec((1, bd, hk, 128), lambda k: (layer, k, 0, 0)),
                  pl.BlockSpec((1, bd, hk, 128), lambda k: (layer, k, 0, 0)),
                  pl.BlockSpec((T, 128), lambda k: (0, 0)), pl.BlockSpec((T, 128), lambda k: (0, 0))],
        out_specs=[pl.BlockSpec((T, nq), lambda k: (0, 0)), pl.BlockSpec((T, 2 * nkv), lambda k: (0, 0))],
        out_shape=[jax.ShapeDtypeStruct((T, nq), BF16), jax.ShapeDtypeStruct((T, 2 * nkv), BF16)],
        scratch_shapes=[pltpu.VMEM((T, nq + 2 * nkv), F32)], name="qkv",
        cost_estimate=pl.CostEstimate(flops=2 * T * D * (nq + 2 * nkv), bytes_accessed=D * (nq + 2 * nkv) * 2 + T * D * 2, transcendentals=0),
        compiler_params=pltpu.CompilerParams(dimension_semantics=("arbitrary",)))(x, inv, gain, w_q, w_k, w_v, cos, sin)


def rms_inv(wide):
    return lax.rsqrt(jnp.mean(wide * wide, axis=-1, keepdims=True) + NORM_EPS)


def rope_tables(positions, base):
    half = HEAD // 2
    inv_freq = base ** (-jnp.arange(half, dtype=F32) / half)
    angles = positions.astype(F32)[:, None] * inv_freq
    cos, sin = jnp.cos(angles), jnp.sin(angles)
    return jnp.concatenate([cos, cos], 1), jnp.concatenate([-sin, sin], 1)


def solution(mesh):
    sp_size = mesh.shape['sp']

    def swap_tp(v):
        return lax.ppermute(v, 'tp', [(0, 1), (1, 0)])

    def swap_sp(v, bit):
        return lax.ppermute(v, 'sp', [(i, i ^ bit) for i in range(sp_size)])

    def rows(v, start, size):
        return lax.dynamic_slice_in_dim(v, start, size, 0)

    def by_xor(parts, sp):
        stack = jnp.concatenate(parts, 0)
        size = parts[0].shape[0]
        return jnp.concatenate([rows(stack, (n ^ sp) * size, size) for n in range(4)], 0)

    def gather_wo(w, sp):
        quarter = w.shape[0] // 4
        piece = quarter // WO_PIECES
        got = []
        for p in range(WO_PIECES):
            mine = swap_tp(rows(w, sp * quarter + p * piece, piece))
            across = swap_sp(mine, 2)
            near = swap_sp(jnp.concatenate([mine, across], 0), 1)
            got.append([mine, near[:piece], across, near[piece:]])
        parts = [jnp.concatenate([g[d] for g in got], 0) for d in range(4)]
        return by_xor(parts, sp)

    def finish_attention(x, a_own, a_peer, wo_own, wo_peer, gain):
        o = jnp.dot(a_own, wo_own, preferred_element_type=F32) + jnp.dot(a_peer, wo_peer, preferred_element_type=F32)
        x_mid = (x.astype(F32) + o * rms_inv(o) * gain[1]).astype(BF16)
        wide = x_mid.astype(F32)
        return x_mid, (wide * rms_inv(wide) * gain[2]).astype(BF16)

    def mlp(u, w_gate, w_up, w_down):
        gate = jnp.dot(u, w_gate, preferred_element_type=F32)
        up = jnp.dot(u, w_up, preferred_element_type=F32)
        f = (jax.nn.silu(gate) * up).astype(BF16)
        return jnp.dot(f, w_down, preferred_element_type=F32)

    def tail(x, a, ap, wo_own, wo_peer, gain, w_gate, w_up, w_down):
        got = []
        for i in range(CHUNKS):
            x_mid, u = finish_attention(x['peer'][i], a['peer'][i], ap['peer'][i], wo_own, wo_peer, gain)
            got.append(swap_tp(mlp(u, w_gate, w_up, w_down)))
        own, peer = [], []
        for i in range(CHUNKS):
            x_mid, u = finish_attention(x['own'][i], a['own'][i], ap['own'][i], wo_own, wo_peer, gain)
            m = mlp(u, w_gate, w_up, w_down) + got[i]
            out = (x_mid.astype(F32) + m * rms_inv(m) * gain[3]).astype(BF16)
            own.append(out)
            peer.append(swap_tp(out))
        return {'own': own, 'peer': peer}

    def chunked(v):
        n = v.shape[0] // CHUNKS
        return [v[i * n:(i + 1) * n] for i in range(CHUNKS)]

    def device_fn(x_loc, pos_loc, gains, w_q, w_k, w_v, w_o, w_gate, w_up, w_down):
        tp, sp = lax.axis_index('tp'), lax.axis_index('sp')
        seq, d_model = x_loc.shape
        half = seq // 2
        own0, peer0 = tp * half, (1 - tp) * half
        tp_heads = w_q.shape[2]
        wo = w_o.reshape(2, tp_heads * HEAD, d_model)

        wo_peer = gather_wo(wo[0], sp)
        cos, sin = rope_tables(pos_loc, LOCAL_BASE)
        q, kv = qkv(0, x_loc, rms_inv(x_loc.astype(F32)), gains[0, 0][None], w_q, w_k, w_v, cos, sin)
        halo = lax.ppermute(kv[seq - WINDOW:], 'sp', [(i, i + 1) for i in range(sp_size - 1)])
        first = (sp * seq).astype(jnp.int32)[None]
        att = attn_local(first, q, jnp.concatenate([halo, kv], 0))
        a = {'own': chunked(rows(att, own0, half)), 'peer': chunked(rows(att, peer0, half))}
        ap = {'peer': [swap_tp(c) for c in a['own']]}
        ap['own'] = [swap_tp(c) for c in a['peer']]
        x = {'own': chunked(rows(x_loc, own0, half)), 'peer': chunked(rows(x_loc, peer0, half))}
        x = tail(x, a, ap, wo[0], wo_peer, gains[0], w_gate[0], w_up[0], w_down[0])

        kv_heads = w_k.shape[2]
        last = sp_size - 1
        tail_kv = kv[seq - WINDOW:]
        pick = lambda n: jnp.concatenate([tail_kv[:, n * HEAD:(n + 1) * HEAD], tail_kv[:, (kv_heads + n) * HEAD:(kv_heads + n + 1) * HEAD]], 1)
        sent = [lax.ppermute(pick(n), 'sp', [(last, n)]) for n in range(last)]
        local = pick(last)
        for n in range(last):
            local = jnp.where(sp == n, sent[n], local)
        k_local, v_local = local[:, None, :HEAD], local[:, None, HEAD:]

        wo_late, _ = lax.optimization_barrier((wo[1], x['own'][-1]))
        wo_peer = gather_wo(wo_late, sp)
        qs, kvs = {}, []
        for side, start in (('own', own0), ('peer', peer0)):
            cos, sin = rope_tables(rows(pos_loc, start, half), GLOBAL_BASE)
            xs = jnp.concatenate(x[side], 0)
            qs[side], kv = qkv(1, xs, rms_inv(xs.astype(F32)), gains[1, 0][None], w_q, w_k, w_v, cos, sin)
            kvs.append(kv)
        mine = jnp.concatenate(kvs, 0)
        across = swap_sp(mine, 2)
        near = swap_sp(jnp.concatenate([mine, across], 0), 1)
        kv_all = jnp.concatenate([mine, near[:seq], across, near[seq:]], 0)
        code = (2 * sp + tp).astype(jnp.int32)
        a, ap = {}, {}
        for side, other, start in (('own', 'peer', own0), ('peer', 'own', peer0)):
            starts = sp * seq + start + jnp.arange(half // Q_ROWS, dtype=jnp.int32) * Q_ROWS
            att = attn_global(jnp.concatenate([code[None], starts.astype(jnp.int32)]), qs[side], kv_all)
            a[side] = chunked(att)
            ap[other] = [swap_tp(c) for c in a[side]]
        x = tail(x, a, ap, wo[1], wo_peer, gains[1], w_gate[1], w_up[1], w_down[1])

        def cache(column):
            blocks = [lax.dynamic_slice(kv_all, ((b ^ code) * half, column), (half, HEAD)) for b in range(2 * sp_size)]
            return jnp.concatenate(blocks, 0)[:, None, :]

        k_global, v_global = cache(sp * HEAD), cache((kv_heads + sp) * HEAD)
        out = jnp.zeros((seq, d_model), BF16)
        n = half // CHUNKS
        for i in range(CHUNKS):
            out = lax.dynamic_update_slice_in_dim(out, x['own'][i], own0 + i * n, 0)
            out = lax.dynamic_update_slice_in_dim(out, x['peer'][i], peer0 + i * n, 0)
        return out, k_local, v_local, k_global, v_global

    token_spec = P(('rep', 'sp'), None)
    cache_spec = P('rep', ('tp', 'sp'), None)
    in_specs = (token_spec, P(('rep', 'sp')), P(), P(None, None, 'tp', None), P(None, None, 'tp', None),
                P(None, None, 'tp', None), P(None, 'tp', None, None), P(None, None, 'tp'), P(None, None, 'tp'),
                P(None, 'tp', None))
    out_specs = (token_spec, cache_spec, cache_spec, cache_spec, cache_spec)
    return jax.shard_map(device_fn, mesh=mesh, in_specs=in_specs, out_specs=out_specs, check_vma=False)
```
